128 devices in a mesh: row: 8 (over z, x_hi), col: 16 (over y, x_lo, core).
Axes of the slice: x: 4 (x_hi: 2, x_lo: 2; x = x_hi * 2 + x_lo), y: 4, z: 4, core: 2. Of those that a mesh axis runs over, the one named last changes fastest.
Arguments:
- t_amps: bfloat16 [16, 16, 128, 128], P('row', 'col'), may hold values from -6 to 6
- df_slabs: bfloat16 [1024, 128, 128], P('col'), may hold values from -0.09375 to 0.09375
- drive: bfloat16 [16, 16, 128, 128], P('row', 'col'), may hold values from -6 to 6
- hole_ints: bfloat16 [16, 16, 16, 16], replicated, may hold values from -0.375 to 0.375
- eps_occ: float32 [16], replicated, may hold values from -0.8 to -0.2
- eps_vir: float32 [128], replicated, may hold values from 0.2 to 1.2
Outputs:
- new_amps: float32 [16, 16, 128, 128], P('row', 'col')
The draws below stay inside these ranges and needn't reach their ends.
All inputs are finite; a program needn't handle non-finite values.
Results may differ from the reference program's by a relative error of at most 0.0095.
Values may be sent and summed in bfloat16 or wider, within the bound.
No kernel may reach another device: no remote copies, remote signals or barrier semaphores. Data moves between devices by JAX's collectives and lax.ppermute only.
A program may use at most 64 MiB of HBM per device.

```python
import jax
import jax.numpy as jnp
from jax import lax

O = 16
V = 128
NQ = 1024


def level_of(key, extent, shards, smallest, high):
    factor_of = 1.0
    for position, parts in shards:
        steps = jax.random.uniform(jax.random.fold_in(jax.random.fold_in(key, 6), position), (parts,), jnp.float32, smallest / len(shards), high / len(shards))
        factor_of = factor_of * jnp.repeat(jnp.exp(steps), extent[position] // parts).reshape((-1,) + (1,) * (len(extent) - 1 - position))
    return factor_of


def normal_values(own_key, shape, width, reach, shards=(), kind=jnp.bfloat16):
    drawn = jax.random.normal(own_key, shape, jnp.float32) * width
    if len(shards) > 0:
        drawn = level_of(own_key, shape, shards, -0.22, 0.18) * drawn
    return jnp.clip(drawn, min=-reach, max=reach).astype(kind)


def setup_inputs(seed: int = 0) -> dict:
    keys = jax.random.split(jax.random.key(seed), 7)
    return {
        "t_amps": normal_values(keys[0], (O, O, V, V), 1.0, 6.0, ((0, 8), (1, 16))),
        "df_slabs": normal_values(keys[1], (NQ, V, V), (V * 32) ** -0.5, 0.09375, ((0, 16),)),
        "drive": normal_values(keys[2], (O, O, V, V), 1.0, 6.0, ((0, 8), (1, 16))),
        "hole_ints": normal_values(keys[3], (O, O, O, O), (O * O) ** -0.5, 0.375),
        "eps_occ": jnp.clip(jax.random.uniform(keys[4], (O,), jnp.float32, -0.8, -0.2), -0.8, -0.2),
        "eps_vir": jnp.clip(jax.random.uniform(keys[5], (V,), jnp.float32, 0.2, 1.2), 0.2, 1.2),
    }


def reference(t_amps, df_slabs, drive, hole_ints, eps_occ, eps_vir):
    slabs = df_slabs.astype(jnp.float32)
    flat_slabs = slabs.reshape(NQ * V, V)
    right_side = jnp.transpose(slabs, (1, 0, 2)).reshape(V, NQ * V)

    def one_pair(amps):
        inner = jnp.dot(flat_slabs, amps.astype(jnp.float32))
        inner = lax.optimization_barrier(inner.astype(jnp.bfloat16)).astype(jnp.float32)
        left_side = jnp.transpose(inner.reshape(NQ, V, V), (1, 0, 2)).reshape(V, NQ * V)
        return jnp.dot(left_side, right_side.T)

    particle = lax.map(one_pair, t_amps.reshape(O * O, V, V)).reshape(O, O, V, V)
    hole = jnp.dot(hole_ints.reshape(O * O, O * O), t_amps.reshape(O * O, V * V), preferred_element_type=jnp.float32)
    hole = lax.optimization_barrier(hole.astype(jnp.bfloat16)).astype(jnp.float32).reshape(O, O, V, V)
    denom = eps_vir[None, None, :, None] + eps_vir[None, None, None, :] - eps_occ[:, None, None, None] - eps_occ[None, :, None, None]
    return (drive.astype(jnp.float32) + particle + hole) / denom
```

```python
import jax
import jax.numpy as jnp
from jax import lax
from jax.experimental import pallas as pl
from jax.experimental.pallas import tpu as pltpu
from jax.sharding import PartitionSpec as P

V = 128
BF = jnp.bfloat16
F32 = jnp.float32
VMEM = pl.BlockSpec(memory_space=pltpu.VMEM)
SMEM = pl.BlockSpec(memory_space=pltpu.SMEM)
SLOTS = [(dy, dx) for dy in range(4) for dx in range(2)]
CHUNK = 16


def peer(c, dy, dx):
    return (((c >> 2) + dy) % 4) * 4 + ((((c >> 1) & 1) ^ dx) << 1) + (c & 1)


def to_peer(x, dy, dx):
    return lax.ppermute(x, "col", [(c, peer(c, dy, dx)) for c in range(16)])


def to_partner(x):
    return lax.ppermute(x, "col", [(c, c ^ 1) for c in range(16)])


def to_row(x, dr):
    return lax.ppermute(x, "row", [(r, (r + dr) % 8) for r in range(8)])


def params(mib=40):
    return pltpu.CompilerParams(vmem_limit_bytes=mib * 2**20)


def cost(flops, nbytes):
    return pl.CostEstimate(flops=flops, bytes_accessed=nbytes, transcendentals=0)


def ladder(amps, slabs, starts, kinds, hole=None, where=None):
    nslot = len(amps)
    pairs = 2 * nslot
    duos = nslot
    nq = slabs.shape[0]
    half = CHUNK // 2
    steps = nq // CHUNK
    nstart = len(starts)
    counts = [s.shape[0] for s in starts]
    merged = len(kinds) == 1

    def kern(*refs):
        refs = list(refs)
        w_ref = refs.pop(0) if where is not None else None
        t_refs, refs = refs[:nslot], refs[nslot:]
        b_ref = refs.pop(0)
        s_refs, refs = refs[:nstart], refs[nstart:]
        h_ref = refs.pop(0) if hole is not None else None
        o_refs, refs = refs[: len(kinds)], refs[len(kinds) :]
        t_ref, xa, xb, acc_ref = refs
        for s in range(nslot):
            t_ref[s * 2 * V : (s + 1) * 2 * V, :] = t_refs[s][...].reshape(2 * V, V)
        if nstart:
            flat = [(ref, p) for ref, n in zip(s_refs, counts) for p in range(n)]
            for p, (ref, at) in enumerate(flat):
                acc_ref[p // 2, :, (p % 2) * V : (p % 2 + 1) * V] = ref[at]
        else:
            acc_ref[...] = jnp.zeros((duos, V, 2 * V), F32)

        def first(k, q, x_ref):
            two = b_ref[pl.ds(k * CHUNK + 2 * q, 2)].reshape(2 * V, V)
            x = lax.dot_general(
                t_ref[...], two, (((1,), (1,)), ((), ())), preferred_element_type=F32
            ).astype(BF)
            for p in range(pairs):
                xp = x[p * V : (p + 1) * V]
                g, h = p // 2, p % 2
                x_ref[g, 2 * q * V : (2 * q + 1) * V, h * V : (h + 1) * V] = xp[:, :V]
                x_ref[g, (2 * q + 1) * V : (2 * q + 2) * V, h * V : (h + 1) * V] = xp[:, V:]

        def second(k, g, x_ref):
            wide = jnp.concatenate([b_ref[k * CHUNK + q] for q in range(CHUNK)], axis=1)
            acc_ref[g] += jnp.dot(wide, x_ref[g], preferred_element_type=F32)

        def both(k1, x1, k2, x2):
            n = max(half, duos)
            for i in range(n):
                for q in range(i * half // n, (i + 1) * half // n):
                    first(k1, q, x1)
                for g in range(i * duos // n, (i + 1) * duos // n):
                    second(k2, g, x2)

        for q in range(half):
            first(0, q, xa)

        def step(m, carry):
            both(2 * m + 1, xb, 2 * m, xa)
            both(2 * m + 2, xa, 2 * m + 1, xb)
            return carry

        lax.fori_loop(0, (steps - 2) // 2, step, 0)
        both(steps - 1, xb, steps - 2, xa)
        for g in range(duos):
            second(steps - 1, g, xb)
            if h_ref is not None:
                rows = pl.ds(pl.multiple_of(w_ref[0] * 16, 16), 16)
                for h in range(2):
                    acc_ref[g, rows, h * V : (h + 1) * V] += h_ref[2 * g + h]
            for h in range(2):
                value = acc_ref[g, :, h * V : (h + 1) * V]
                if merged:
                    o_refs[0][2 * g + h] = value.astype(kinds[0])
                else:
                    o_refs[g][h] = value.astype(kinds[g])

    args = list(amps) + [slabs] + list(starts) + ([hole] if hole is not None else [])
    specs = [VMEM] * len(args)
    if where is not None:
        args, specs = [where] + args, [SMEM] + specs
    if merged:
        shapes = [jax.ShapeDtypeStruct((pairs, V, V), kinds[0])]
    else:
        shapes = [jax.ShapeDtypeStruct((2, V, V), kind) for kind in kinds]
    return pl.pallas_call(
        kern,
        in_specs=specs,
        out_specs=[VMEM] * len(shapes),
        out_shape=shapes,
        scratch_shapes=[pltpu.VMEM((pairs * V, V), BF)]
        + [pltpu.VMEM((duos, CHUNK * V, 2 * V), BF)] * 2
        + [pltpu.VMEM((duos, V, 2 * V), F32)],
        compiler_params=params(),
        cost_estimate=cost(4 * pairs * nq * V**3, slabs.size * 2),
        name=f"ladder{nslot}",
    )(*args)


def cut_slices(amps, where):
    def kern(w_ref, *refs):
        t_refs, o_ref, scr = refs[:8], refs[8], refs[9]
        rows = pl.ds(pl.multiple_of(w_ref[0] * 16, 16), 16)
        for s in range(8):
            for k in range(2):
                scr[:, 2 * s + k, :] = t_refs[s][k, rows, :].astype(F32)
        o_ref[...] = scr[...].astype(BF)

    return pl.pallas_call(
        kern,
        in_specs=[SMEM] + [VMEM] * 8,
        out_specs=VMEM,
        out_shape=jax.ShapeDtypeStruct((16, 16, V), BF),
        scratch_shapes=[pltpu.VMEM((16, 16, V), F32)],
        compiler_params=params(),
        cost_estimate=cost(10**6, 10**5),
        name="cut_slices",
    )(where, *amps)


def hole_and_finish(mine, other, ints, where, partial):
    def kern(*refs):
        w_ref, refs = refs[0], refs[1:]
        m_refs, p_refs, refs = refs[:8], refs[8:16], refs[16:]
        h_ref, d_ref, out_ref, o_refs, scr = refs[0], refs[1], refs[2], refs[3:7], refs[7]
        m, r, c = w_ref[0], w_ref[1], w_ref[2]
        y, xl, core = c >> 2, (c >> 1) & 1, c & 1

        def column(slot):
            dy, dx = slot >> 1, slot & 1
            return (((y - dy) & 3) << 2) + ((xl ^ dx) << 1) + core

        true = lax.broadcasted_iota(jnp.int32, (256, 256), 0)
        here = lax.broadcasted_iota(jnp.int32, (256, 256), 1)
        flip, dr, slot, kk = here >> 7, (here >> 4) & 7, (here >> 1) & 7, here & 1
        wanted = ((((r - dr) & 7) * 2 + kk) << 4) + (column(slot) ^ flip)
        pick = jnp.where(true == wanted, 1.0, 0.0).astype(BF)
        ordered = jnp.dot(h_ref[...], pick, preferred_element_type=F32).astype(BF)
        line = lax.broadcasted_iota(jnp.int32, (16, 32), 0)
        pair = lax.broadcasted_iota(jnp.int32, (16, 32), 1)
        take = jnp.where(pair == ((line & 1) << 4) + column(line >> 1), 1.0, 0.0).astype(BF)
        weights = jnp.dot(take, ordered, preferred_element_type=F32).astype(BF)
        for a in range(16):
            stack = jnp.concatenate([ref[a] for ref in m_refs] + [ref[a] for ref in p_refs], axis=0)
            scr[a] = jnp.dot(weights, stack, preferred_element_type=F32)
        rows = pl.ds(pl.multiple_of(m * 16, 16), 16)
        for n in range(16):
            out_ref[n] = scr[:, n, :]
        for s in range(4):
            for k in range(2):
                o_refs[s][k] = d_ref[2 * s + k].astype(BF)
                o_refs[s][k, rows, :] = (d_ref[2 * s + k, rows, :] + scr[:, 8 + 2 * s + k, :]).astype(BF)

    return pl.pallas_call(
        kern,
        in_specs=[SMEM] + [VMEM] * 18,
        out_specs=[VMEM] * 5,
        out_shape=[jax.ShapeDtypeStruct((16, 16, V), F32)]
        + [jax.ShapeDtypeStruct((2, V, V), BF)] * 4,
        scratch_shapes=[pltpu.VMEM((16, 16, V), F32)],
        compiler_params=params(),
        cost_estimate=cost(10**8, 10**6),
        name="hole_and_finish",
    )(where, *mine, *other, ints, partial)


def body(t_amps, df_slabs, drive, hole_ints, eps_occ, eps_vir):
    r = lax.axis_index("row")
    c = lax.axis_index("col")
    where = jnp.stack([c >> 1, r, c]).astype(jnp.int32)
    own = t_amps.reshape(2, V, V)
    amps = [own] + [to_peer(own, dy, dx) for dy, dx in SLOTS[1:]]
    others = to_partner(df_slabs)
    ints = lax.dynamic_slice_in_dim(hole_ints, r * 2, 2, 0).reshape(32, 256)
    part_a = ladder(amps[:1], df_slabs, [], [F32])[0]
    part_b = ladder(amps[1:4], df_slabs, [], [F32])[0]
    slices = cut_slices(amps, where)
    part_c = ladder(amps[4:], df_slabs, [], [F32])[0]
    mine = [slices] + [to_row(slices, dr) for dr in range(1, 8)]
    partners = [to_partner(piece) for piece in mine]
    part_d = ladder(amps[4:], others, [part_c], [F32])[0]
    hole, *done_d = hole_and_finish(mine, partners, ints, where, part_d)
    total, *done_e = ladder(
        amps[:4], others, [part_a, part_b], [F32, BF, BF, BF], hole=hole, where=where
    )
    back = {}
    for s, value in list(zip(range(4, 8), done_d)) + list(zip(range(1, 4), done_e)):
        dy, dx = SLOTS[s]
        back[s] = to_peer(value, -dy, dx)
    for s in range(1, 8):
        total = total + back[s].astype(F32)
    occ_first = lax.dynamic_slice_in_dim(eps_occ, r * 2, 2, 0)
    occ_second = lax.dynamic_slice_in_dim(eps_occ, c, 1, 0)
    denom = (
        eps_vir[None, :, None]
        + eps_vir[None, None, :]
        - occ_first[:, None, None]
        - occ_second[:, None, None]
    )
    return ((drive.reshape(2, V, V).astype(F32) + total) / denom).reshape(2, 1, V, V)


def solution(mesh):
    placed = (
        P("row", "col", None, None),
        P("col", None, None),
        P("row", "col", None, None),
        P(),
        P(),
        P(),
    )
    return jax.shard_map(
        body, mesh=mesh, in_specs=placed, out_specs=P("row", "col", None, None), check_vma=False
    )
```

```python
import jax
import jax.numpy as jnp
from jax import lax
from jax.experimental import pallas as pl
from jax.experimental.pallas import tpu as pltpu
from jax.sharding import PartitionSpec as P


V = 128
BF = jnp.bfloat16
F32 = jnp.float32
VMEM = pl.BlockSpec(memory_space=pltpu.VMEM)
SMEM = pl.BlockSpec(memory_space=pltpu.SMEM)
ANY = pl.BlockSpec(memory_space=pl.ANY)
CHUNK = 8
PARTS = 4


def col_swap(x, mask):
    return lax.ppermute(x, "col", [(c, c ^ mask) for c in range(16)])


def row_swap(x, mask):
    return lax.ppermute(x, "row", [(r, r ^ mask) for r in range(8)])


def params(mib=48):
    return pltpu.CompilerParams(vmem_limit_bytes=mib * 2**20)


def cost(flops, nbytes):
    return pl.CostEstimate(flops=flops, bytes_accessed=nbytes, transcendentals=0)


def ladder(amps, slabs, starts, fetch=False, kind=F32):
    pairs = amps.shape[0]
    duos = pairs // 2
    nq = slabs.shape[0]
    half = CHUNK // 2
    steps = nq // CHUNK
    nstart = len(starts)
    part = nq // PARTS
    offsets = [at for _, at in starts]

    def kern(*refs):
        refs = list(refs)
        t_ref, src_ref = refs[:2]
        s_refs, refs = refs[2 : 2 + nstart], refs[2 + nstart :]
        o_ref = refs.pop(0)
        b_ref = refs.pop(0) if fetch else src_ref
        xa, xb, acc_ref = refs[:3]
        copies = []
        if fetch:
            sems = refs[3]
            for n in range(PARTS):
                span = pl.ds(n * part, part)
                copies.append(pltpu.make_async_copy(src_ref.at[span], b_ref.at[span], sems.at[n]))
                copies[-1].start()
        for p in range(pairs):
            cols = slice((p % 2) * V, (p % 2 + 1) * V)
            if nstart:
                value = s_refs[0][offsets[0] + p]
                for ref, at in zip(s_refs[1:], offsets[1:]):
                    value = value + ref[at + p]
            else:
                value = jnp.zeros((V, V), F32)
            acc_ref[p // 2, :, cols] = value

        def first(k, q, x_ref):
            two = b_ref[pl.ds(k * CHUNK + 2 * q, 2)].reshape(2 * V, V)
            x = lax.dot_general(
                t_ref[...].reshape(pairs * V, V),
                two,
                (((1,), (1,)), ((), ())),
                preferred_element_type=F32,
            ).astype(BF)
            for p in range(pairs):
                xp = x[p * V : (p + 1) * V]
                g, h = p // 2, p % 2
                x_ref[g, 2 * q * V : (2 * q + 1) * V, h * V : (h + 1) * V] = xp[:, :V]
                x_ref[g, (2 * q + 1) * V : (2 * q + 2) * V, h * V : (h + 1) * V] = xp[:, V:]

        def second(k, g, x_ref):
            wide = jnp.concatenate([b_ref[k * CHUNK + q] for q in range(CHUNK)], axis=1)
            acc_ref[g] += jnp.dot(wide, x_ref[g], preferred_element_type=F32)

        def both(k1, x1, k2, x2):
            n = max(half, duos)
            for i in range(n):
                for q in range(i * half // n, (i + 1) * half // n):
                    first(k1, q, x1)
                for g in range(i * duos // n, (i + 1) * duos // n):
                    second(k2, g, x2)

        if fetch:
            copies[0].wait()
        for q in range(half):
            first(0, q, xa)
        if fetch:
            for copy in copies[1:]:
                copy.wait()

        def step(m, carry):
            both(2 * m + 1, xb, 2 * m, xa)
            both(2 * m + 2, xa, 2 * m + 1, xb)
            return carry

        lax.fori_loop(0, (steps - 2) // 2, step, 0)
        both(steps - 1, xb, steps - 2, xa)
        for g in range(duos):
            second(steps - 1, g, xb)
        for p in range(pairs):
            o_ref[p] = acc_ref[p // 2, :, (p % 2) * V : (p % 2 + 1) * V].astype(kind)

    shapes = [jax.ShapeDtypeStruct((pairs, V, V), kind)]
    scratch = [pltpu.VMEM((duos, CHUNK * V, 2 * V), BF)] * 2 + [pltpu.VMEM((duos, V, 2 * V), F32)]
    if fetch:
        shapes.append(jax.ShapeDtypeStruct(slabs.shape, BF))
        scratch.append(pltpu.SemaphoreType.DMA((PARTS,)))
    out = pl.pallas_call(
        kern,
        in_specs=[VMEM, ANY if fetch else VMEM] + [VMEM] * nstart,
        out_specs=[VMEM] * len(shapes),
        out_shape=shapes,
        scratch_shapes=scratch,
        compiler_params=params(),
        cost_estimate=cost(4 * pairs * nq * V**3, slabs.size * 2),
    )(amps, slabs, *[s for s, _ in starts])
    return out if fetch else out[0]


def spread_ints(ints, where):
    def kern(w_ref, h_ref, o_ref):
        r, c = w_ref[0], w_ref[1]
        line = lax.broadcasted_iota(jnp.int32, (256, 32), 0) >> 4
        pair = lax.broadcasted_iota(jnp.int32, (256, 32), 1)
        g, ii = line >> 1, line & 1
        slot = ((g & 1) << 2) | (g & 2) | (g >> 2)
        rows = jnp.where(pair == (ii << 4) + (c ^ (slot << 1)), 1.0, 0.0).astype(BF)
        picked = jnp.dot(rows, h_ref[...], preferred_element_type=F32).astype(BF)
        true = lax.broadcasted_iota(jnp.int32, (256, 512), 0)
        here = lax.broadcasted_iota(jnp.int32, (256, 512), 1)
        par, d, kk = here >> 8, (here >> 5) & 7, (here >> 4) & 1
        mask = (d & 1) | ((d & 2) << 1) | ((d & 4) >> 1)
        wanted = ((((r ^ mask) << 1) + kk) << 4) + (c ^ par)
        cols = jnp.where(true == wanted, 1.0, 0.0).astype(BF)
        wide = jnp.dot(picked, cols, preferred_element_type=F32)
        o_ref[...] = jnp.where((true & 15) == (here & 15), wide, 0.0).astype(BF)

    return pl.pallas_call(
        kern,
        in_specs=[SMEM, VMEM],
        out_specs=VMEM,
        out_shape=jax.ShapeDtypeStruct((256, 512), BF),
        compiler_params=params(),
        cost_estimate=cost(10**8, 10**6),
        name="spread",
    )(where, ints)


def hole_terms(wide, mine, other):
    def kern(w_ref, m_ref, p_ref, o_ref):
        for ga in range(8):
            rows = slice(ga * 16, (ga + 1) * 16)
            stack = jnp.concatenate(
                [m_ref[q, rows, :] for q in range(16)] + [p_ref[q, rows, :] for q in range(16)],
                axis=0,
            )
            terms = jnp.dot(w_ref[...], stack, preferred_element_type=F32)
            for n in range(16):
                o_ref[n, rows, :] = terms[n * 16 : (n + 1) * 16]

    return pl.pallas_call(
        kern,
        in_specs=[VMEM] * 3,
        out_specs=VMEM,
        out_shape=jax.ShapeDtypeStruct((16, V, V), F32),
        compiler_params=params(),
        cost_estimate=cost(10**9, 10**6),
        name="hole",
    )(wide, mine, other)


def body(t_amps, df_slabs, drive, hole_ints, eps_occ, eps_vir):
    r = lax.axis_index("row")
    c = lax.axis_index("col")
    where = jnp.stack([r, c]).astype(jnp.int32)
    own = t_amps.reshape(2, V, V)
    others = col_swap(df_slabs, 1)
    got_y2 = col_swap(own, 8)
    rows1 = row_swap(own, 1)
    ints = lax.dynamic_slice_in_dim(hole_ints, r * 2, 2, 0).reshape(32, 256)
    wide = spread_ints(ints, where)
    part_0, slabs = ladder(own, df_slabs, [], True)
    near = jnp.concatenate([own, got_y2])
    got_y1 = col_swap(near, 4)
    two_rows = jnp.concatenate([own, rows1])
    rows2 = row_swap(two_rows, 4)
    part_4 = ladder(got_y2, slabs, [])
    got_x = col_swap(jnp.concatenate([near, got_y1]), 2)
    four_rows = jnp.concatenate([two_rows, rows2])
    rows3 = row_swap(four_rows, 2)
    part_26 = ladder(got_y1, slabs, [])
    mine = jnp.concatenate([four_rows, rows3])
    other = col_swap(mine, 1)
    part_x = ladder(got_x, slabs, [])
    hole = hole_terms(wide, mine, other)
    send_x, fetched = ladder(got_x, others, [(part_x, 0), (hole, 8)], True, BF)
    back_x = col_swap(send_x, 2).astype(F32)
    full_26 = ladder(got_y1, fetched, [(part_26, 0), (hole, 4)])
    back_y1 = col_swap((full_26 + back_x[4:]).astype(BF), 4).astype(F32)
    start_04 = jnp.concatenate([part_0, part_4])
    full_04 = ladder(near, fetched, [(start_04, 0), (hole, 0)])
    total = full_04 + back_x[:4] + back_y1
    back_y2 = col_swap(total[2:].astype(BF), 8).astype(F32)
    total = total[:2] + back_y2
    occ_first = lax.dynamic_slice_in_dim(eps_occ, r * 2, 2, 0)
    occ_second = lax.dynamic_slice_in_dim(eps_occ, c, 1, 0)
    denom = (
        eps_vir[None, :, None]
        + eps_vir[None, None, :]
        - occ_first[:, None, None]
        - occ_second[:, None, None]
    )
    return ((drive.reshape(2, V, V).astype(F32) + total) / denom).reshape(2, 1, V, V)


def solution(mesh):
    placed = (
        P("row", "col", None, None),
        P("col", None, None),
        P("row", "col", None, None),
        P(),
        P(),
        P(),
    )

    return jax.shard_map(
        body, mesh=mesh, in_specs=placed, out_specs=P("row", "col", None, None), check_vma=False
    )
```

```python
import jax
import jax.numpy as jnp
from jax import lax
from jax.experimental import pallas as pl
from jax.experimental.pallas import tpu as pltpu
from jax.sharding import PartitionSpec as P


V = 128
BF = jnp.bfloat16
F32 = jnp.float32
VMEM = pl.BlockSpec(memory_space=pltpu.VMEM)
SMEM = pl.BlockSpec(memory_space=pltpu.SMEM)
HBM = pl.BlockSpec(memory_space=pltpu.HBM)
PARTS = 8


def col_swap(x, mask):
    return lax.ppermute(x, "col", [(c, c ^ mask) for c in range(16)])


def row_swap(x, mask):
    return lax.ppermute(x, "row", [(r, r ^ mask) for r in range(8)])


def params(mib):
    return pltpu.CompilerParams(vmem_limit_bytes=mib * 2**20)


def cost(flops, nbytes):
    return pl.CostEstimate(flops=flops, bytes_accessed=nbytes, transcendentals=0)


def ladder(amps, slabs, starts, pairs, at=0, fetch=False, give=False, kind=F32, chunk=8):
    duos = pairs // 2
    nq = slabs.shape[0]
    half = chunk // 2
    steps = nq // chunk
    nstart = len(starts)
    part = nq // PARTS
    offsets = [n for _, n in starts]

    def kern(*refs):
        refs = list(refs)
        t_ref, src_ref = refs[:2]
        s_refs, refs = refs[2 : 2 + nstart], refs[2 + nstart :]
        o_ref = refs.pop(0)
        b_ref = refs.pop(0) if give else refs[4] if fetch else src_ref
        xa, xb, acc_ref = refs[:3]
        copies = []
        if fetch:
            sems = refs[3]
            for n in range(PARTS):
                span = pl.ds(n * part, part)
                copies.append(pltpu.make_async_copy(src_ref.at[span], b_ref.at[span], sems.at[n]))
                copies[-1].start()
        for p in range(pairs):
            cols = slice((p % 2) * V, (p % 2 + 1) * V)
            if nstart:
                value = s_refs[0][offsets[0] + p]
                for ref, n in zip(s_refs[1:], offsets[1:]):
                    value = value + ref[n + p]
            else:
                value = jnp.zeros((V, V), F32)
            acc_ref[p // 2, :, cols] = value

        def first(k, q, x_ref):
            two = b_ref[pl.ds(k * chunk + 2 * q, 2)].reshape(2 * V, V)
            x = lax.dot_general(
                t_ref[at : at + pairs].reshape(pairs * V, V),
                two,
                (((1,), (1,)), ((), ())),
                preferred_element_type=F32,
            ).astype(BF)
            for p in range(pairs):
                xp = x[p * V : (p + 1) * V]
                g, h = p // 2, p % 2
                x_ref[g, 2 * q * V : (2 * q + 1) * V, h * V : (h + 1) * V] = xp[:, :V]
                x_ref[g, (2 * q + 1) * V : (2 * q + 2) * V, h * V : (h + 1) * V] = xp[:, V:]

        def second(k, g, x_ref):
            wide = jnp.concatenate([b_ref[k * chunk + q] for q in range(chunk)], axis=1)
            acc_ref[g] += jnp.dot(wide, x_ref[g], preferred_element_type=F32)

        def both(k1, x1, k2, x2):
            n = max(half, duos)
            for i in range(n):
                for q in range(i * half // n, (i + 1) * half // n):
                    first(k1, q, x1)
                for g in range(i * duos // n, (i + 1) * duos // n):
                    second(k2, g, x2)

        ahead = max(1, chunk // part)
        for copy in copies[:ahead]:
            copy.wait()
        for q in range(half):
            first(0, q, xa)
        for copy in copies[ahead:]:
            copy.wait()

        def step(m, carry):
            both(2 * m + 1, xb, 2 * m, xa)
            both(2 * m + 2, xa, 2 * m + 1, xb)
            return carry

        lax.fori_loop(0, (steps - 2) // 2, step, 0)
        both(steps - 1, xb, steps - 2, xa)
        for g in range(duos):
            second(steps - 1, g, xb)
        for p in range(pairs):
            o_ref[p] = acc_ref[p // 2, :, (p % 2) * V : (p % 2 + 1) * V].astype(kind)

    shapes = [jax.ShapeDtypeStruct((pairs, V, V), kind)]
    scratch = [pltpu.VMEM((duos, chunk * V, 2 * V), BF)] * 2 + [pltpu.VMEM((duos, V, 2 * V), F32)]
    if fetch:
        slabs = pltpu.with_memory_space_constraint(slabs, pltpu.HBM)
        scratch.append(pltpu.SemaphoreType.DMA((PARTS,)))
    if give:
        shapes.append(jax.ShapeDtypeStruct(slabs.shape, BF))
    elif fetch:
        scratch.append(pltpu.VMEM(slabs.shape, BF))
    out = pl.pallas_call(
        kern,
        in_specs=[VMEM, HBM if fetch else VMEM] + [VMEM] * nstart,
        out_specs=[VMEM] * len(shapes),
        out_shape=shapes,
        scratch_shapes=scratch,
        compiler_params=params(8 + duos * chunk * 256 // 1024),
        cost_estimate=cost(4 * pairs * nq * V**3, slabs.size * 2),
    )(amps, slabs, *[s for s, _ in starts])
    return out if give else out[0]


def spread_ints(ints, where):
    def kern(w_ref, h_ref, o_ref):
        r, c = w_ref[0], w_ref[1]
        line = lax.broadcasted_iota(jnp.int32, (256, 32), 0) >> 4
        pair = lax.broadcasted_iota(jnp.int32, (256, 32), 1)
        g, ii = line >> 1, line & 1
        slot = ((g & 1) << 2) | (g & 2) | (g >> 2)
        rows = jnp.where(pair == (ii << 4) + (c ^ (slot << 1)), 1.0, 0.0).astype(BF)
        picked = jnp.dot(rows, h_ref[...], preferred_element_type=F32).astype(BF)
        true = lax.broadcasted_iota(jnp.int32, (256, 512), 0)
        here = lax.broadcasted_iota(jnp.int32, (256, 512), 1)
        par, d, kk = here >> 8, (here >> 5) & 7, (here >> 4) & 1
        mask = (d & 1) | ((d & 2) << 1) | ((d & 4) >> 1)
        wanted = ((((r ^ mask) << 1) + kk) << 4) + (c ^ par)
        cols = jnp.where(true == wanted, 1.0, 0.0).astype(BF)
        wide = jnp.dot(picked, cols, preferred_element_type=F32)
        o_ref[...] = jnp.where((true & 15) == (here & 15), wide, 0.0).astype(BF)

    return pl.pallas_call(
        kern,
        in_specs=[SMEM, VMEM],
        out_specs=VMEM,
        out_shape=jax.ShapeDtypeStruct((256, 512), BF),
        compiler_params=params(8),
        cost_estimate=cost(10**8, 10**6),
        name="spread",
    )(where, ints)


def hole_terms(wide, mine, other):
    def kern(w_ref, m_ref, p_ref, o_ref):
        for ga in range(8):
            rows = slice(ga * 16, (ga + 1) * 16)
            stack = jnp.concatenate(
                [m_ref[q, rows, :] for q in range(16)] + [p_ref[q, rows, :] for q in range(16)],
                axis=0,
            )
            terms = jnp.dot(w_ref[...], stack, preferred_element_type=F32)
            for n in range(16):
                o_ref[n, rows, :] = terms[n * 16 : (n + 1) * 16]

    return pl.pallas_call(
        kern,
        in_specs=[VMEM] * 3,
        out_specs=VMEM,
        out_shape=jax.ShapeDtypeStruct((16, V, V), F32),
        compiler_params=params(8),
        cost_estimate=cost(10**9, 10**6),
        name="hole",
    )(wide, mine, other)


def body(t_amps, df_slabs, drive, hole_ints, eps_occ, eps_vir):
    r = lax.axis_index("row")
    c = lax.axis_index("col")
    where = jnp.stack([r, c]).astype(jnp.int32)
    own = t_amps.reshape(2, V, V)
    others = col_swap(df_slabs, 1)
    got_y2 = col_swap(own, 8)
    rows1 = row_swap(own, 1)
    ints = lax.dynamic_slice_in_dim(hole_ints, r * 2, 2, 0).reshape(32, 256)
    wide = spread_ints(ints, where)
    part_0 = ladder(own, df_slabs, [], 2, fetch=True)
    near = jnp.concatenate([own, got_y2])
    got_y1 = col_swap(near, 4)
    two_rows = jnp.concatenate([own, rows1])
    rows2 = row_swap(two_rows, 4)
    part_4 = ladder(got_y2, df_slabs, [], 2, fetch=True)
    got_x = col_swap(jnp.concatenate([near, got_y1]), 2)
    four_rows = jnp.concatenate([two_rows, rows2])
    rows3 = row_swap(four_rows, 2)
    part_26 = ladder(got_y1, df_slabs, [], 4, fetch=True)
    mine = jnp.concatenate([four_rows, rows3])
    other = col_swap(mine, 1)
    part_x = ladder(got_x, df_slabs, [], 8, fetch=True, chunk=16)
    hole = hole_terms(wide, mine, other)
    send_b, fetched = ladder(
        got_x, others, [(part_x, 4), (hole, 12)], 4, 4, fetch=True, give=True, kind=BF
    )
    back_b = col_swap(send_b, 2).astype(F32)
    send_a = ladder(got_x, fetched, [(part_x, 0), (hole, 8)], 4, 0, kind=BF)
    back_a = col_swap(send_a, 2).astype(F32)
    full_26 = ladder(got_y1, fetched, [(part_26, 0), (hole, 4)], 4)
    back_y1 = col_swap((full_26 + back_b).astype(BF), 4).astype(F32)
    start_04 = jnp.concatenate([part_0, part_4])
    full_04 = ladder(near, fetched, [(start_04, 0), (hole, 0)], 4)
    total = full_04 + back_a + back_y1
    back_y2 = col_swap(total[2:].astype(BF), 8).astype(F32)
    total = total[:2] + back_y2
    occ_first = lax.dynamic_slice_in_dim(eps_occ, r * 2, 2, 0)
    occ_second = lax.dynamic_slice_in_dim(eps_occ, c, 1, 0)
    denom = (
        eps_vir[None, :, None]
        + eps_vir[None, None, :]
        - occ_first[:, None, None]
        - occ_second[:, None, None]
    )
    return ((drive.reshape(2, V, V).astype(F32) + total) / denom).reshape(2, 1, V, V)


def solution(mesh):
    placed = (
        P("row", "col", None, None),
        P("col", None, None),
        P("row", "col", None, None),
        P(),
        P(),
        P(),
    )

    return jax.shard_map(
        body, mesh=mesh, in_specs=placed, out_specs=P("row", "col", None, None), check_vma=False
    )
```

```python
import jax
import jax.numpy as jnp
from jax import lax
from jax.experimental import pallas as pl
from jax.experimental.pallas import tpu as pltpu
from jax.sharding import PartitionSpec as P


V = 128
BF = jnp.bfloat16
F32 = jnp.float32
VMEM = pl.BlockSpec(memory_space=pltpu.VMEM)
SMEM = pl.BlockSpec(memory_space=pltpu.SMEM)
HBM = pl.BlockSpec(memory_space=pltpu.HBM)
PARTS = 8


def col_swap(x, mask):
    return lax.ppermute(x, "col", [(c, c ^ mask) for c in range(16)])


def row_swap(x, mask):
    return lax.ppermute(x, "row", [(r, r ^ mask) for r in range(8)])


def params(mib):
    return pltpu.CompilerParams(vmem_limit_bytes=mib * 2**20)


def cost(flops, nbytes):
    return pl.CostEstimate(flops=flops, bytes_accessed=nbytes, transcendentals=0)


def ladder(amps, slabs, starts, pull=False, kind=F32, chunk=8):
    pairs = sum(n for _, _, n in amps)
    duos = pairs // 2
    nq = slabs.shape[0]
    half = chunk // 2
    steps = nq // chunk
    part = nq // PARTS
    namps = len(amps)
    nstart = sum(len(pieces) for pieces in starts)

    def kern(*refs):
        refs = list(refs)
        t_refs, src_ref = refs[:namps], refs[namps]
        s_refs, refs = refs[namps + 1 : namps + 1 + nstart], refs[namps + 1 + nstart :]
        o_ref = refs.pop(0)
        b_ref = refs.pop(0) if pull else src_ref
        xa, xb, acc_ref, home = refs[:4]
        copies = []
        if pull:
            pulled = pltpu.make_async_copy(t_refs[0], home, refs[5])
            pulled.start()
            for n in range(PARTS):
                span = pl.ds(n * part, part)
                copies.append(pltpu.make_async_copy(src_ref.at[span], b_ref.at[span], refs[4].at[n]))
                copies[-1].start()
        else:
            to = 0
            for ref, (_, at, n) in zip(t_refs, amps):
                home[to : to + n] = ref[at : at + n]
                to += n
        sums = [None] * pairs
        left = list(s_refs)
        for pieces in starts:
            to = 0
            for _, at, n in pieces:
                ref = left.pop(0)
                for p in range(n):
                    value = ref[at + p]
                    sums[to + p] = value if sums[to + p] is None else sums[to + p] + value
                to += n
        for p in range(pairs):
            value = jnp.zeros((V, V), F32) if sums[p] is None else sums[p]
            acc_ref[p // 2, :, (p % 2) * V : (p % 2 + 1) * V] = value

        def first(k, q, x_ref):
            two = b_ref[pl.ds(k * chunk + 2 * q, 2)].reshape(2 * V, V)
            x = lax.dot_general(
                home[...].reshape(pairs * V, V),
                two,
                (((1,), (1,)), ((), ())),
                preferred_element_type=F32,
            ).astype(BF)
            for p in range(pairs):
                xp = x[p * V : (p + 1) * V]
                g, h = p // 2, p % 2
                x_ref[g, 2 * q * V : (2 * q + 1) * V, h * V : (h + 1) * V] = xp[:, :V]
                x_ref[g, (2 * q + 1) * V : (2 * q + 2) * V, h * V : (h + 1) * V] = xp[:, V:]

        def second(k, g, x_ref):
            wide = jnp.concatenate([b_ref[k * chunk + q] for q in range(chunk)], axis=1)
            acc_ref[g] += jnp.dot(wide, x_ref[g], preferred_element_type=F32)

        def both(k1, x1, k2, x2):
            n = max(half, duos)
            for i in range(n):
                for q in range(i * half // n, (i + 1) * half // n):
                    first(k1, q, x1)
                for g in range(i * duos // n, (i + 1) * duos // n):
                    second(k2, g, x2)

        if pull:
            pulled.wait()
        ahead = max(1, chunk // part)
        for copy in copies[:ahead]:
            copy.wait()
        for q in range(half):
            first(0, q, xa)
        for copy in copies[ahead:]:
            copy.wait()

        def step(m, carry):
            both(2 * m + 1, xb, 2 * m, xa)
            both(2 * m + 2, xa, 2 * m + 1, xb)
            return carry

        lax.fori_loop(0, (steps - 2) // 2, step, 0)
        both(steps - 1, xb, steps - 2, xa)
        for g in range(duos):
            second(steps - 1, g, xb)
        for p in range(pairs):
            o_ref[p] = acc_ref[p // 2, :, (p % 2) * V : (p % 2 + 1) * V].astype(kind)

    shapes = [jax.ShapeDtypeStruct((pairs, V, V), kind)]
    scratch = [pltpu.VMEM((duos, chunk * V, 2 * V), BF)] * 2 + [pltpu.VMEM((duos, V, 2 * V), F32)]
    scratch.append(pltpu.VMEM((pairs, V, V), BF))
    arrays = [array for array, _, _ in amps] + [slabs]
    if pull:
        shapes.append(jax.ShapeDtypeStruct(slabs.shape, BF))
        scratch += [pltpu.SemaphoreType.DMA((PARTS,)), pltpu.SemaphoreType.DMA(())]
        arrays = [pltpu.with_memory_space_constraint(array, pltpu.HBM) for array in arrays]
    specs = [HBM if pull else VMEM] * len(arrays) + [VMEM] * nstart
    out = pl.pallas_call(
        kern,
        in_specs=specs,
        out_specs=[VMEM] * len(shapes),
        out_shape=shapes,
        scratch_shapes=scratch,
        compiler_params=params(8 + duos * chunk * 256 // 1024),
        cost_estimate=cost(4 * pairs * nq * V**3, slabs.size * 2),
    )(*arrays, *[array for pieces in starts for array, _, _ in pieces])
    return out if pull else out[0]


def spread_ints(ints, where):
    def kern(w_ref, h_ref, o_ref):
        r, c = w_ref[0], w_ref[1]
        line = lax.broadcasted_iota(jnp.int32, (256, 32), 0) >> 4
        pair = lax.broadcasted_iota(jnp.int32, (256, 32), 1)
        slot, ii = line >> 1, line & 1
        rows = jnp.where(pair == (ii << 4) + (c ^ (slot << 1)), 1.0, 0.0).astype(BF)
        picked = jnp.dot(rows, h_ref[...], preferred_element_type=F32).astype(BF)
        true = lax.broadcasted_iota(jnp.int32, (256, 512), 0)
        here = lax.broadcasted_iota(jnp.int32, (256, 512), 1)
        par, d, kk = here >> 8, (here >> 5) & 7, (here >> 4) & 1
        mask = (d & 1) | ((d & 2) << 1) | ((d & 4) >> 1)
        wanted = ((((r ^ mask) << 1) + kk) << 4) + (c ^ par)
        cols = jnp.where(true == wanted, 1.0, 0.0).astype(BF)
        wide = jnp.dot(picked, cols, preferred_element_type=F32)
        o_ref[...] = jnp.where((true & 15) == (here & 15), wide, 0.0).astype(BF)

    return pl.pallas_call(
        kern,
        in_specs=[SMEM, VMEM],
        out_specs=VMEM,
        out_shape=jax.ShapeDtypeStruct((256, 512), BF),
        compiler_params=params(8),
        cost_estimate=cost(10**8, 10**6),
        name="spread",
    )(where, ints)


def hole_terms(wide, mine, other):
    def kern(w_ref, m_ref, p_ref, o_ref):
        for ga in range(8):
            rows = slice(ga * 16, (ga + 1) * 16)
            stack = jnp.concatenate(
                [m_ref[q, rows, :] for q in range(16)] + [p_ref[q, rows, :] for q in range(16)],
                axis=0,
            )
            terms = jnp.dot(w_ref[...], stack, preferred_element_type=F32)
            for n in range(16):
                o_ref[n, rows, :] = terms[n * 16 : (n + 1) * 16]

    return pl.pallas_call(
        kern,
        in_specs=[VMEM] * 3,
        out_specs=VMEM,
        out_shape=jax.ShapeDtypeStruct((16, V, V), F32),
        compiler_params=params(8),
        cost_estimate=cost(10**9, 10**6),
        name="hole",
    )(wide, mine, other)


def body(t_amps, df_slabs, drive, hole_ints, eps_occ, eps_vir):
    r = lax.axis_index("row")
    c = lax.axis_index("col")
    where = jnp.stack([r, c]).astype(jnp.int32)
    own = t_amps.reshape(2, V, V)
    others = col_swap(df_slabs, 1)
    got_y2 = col_swap(own, 8)
    rows1 = row_swap(own, 1)
    ints = lax.dynamic_slice_in_dim(hole_ints, r * 2, 2, 0).reshape(32, 256)
    first, where, ints = lax.optimization_barrier((own, where, ints))
    wide = spread_ints(ints, where)
    part_0, slabs = ladder([(first, 0, 2)], df_slabs, [], pull=True, chunk=16)
    near = jnp.concatenate([own, got_y2])
    got_y1 = col_swap(near, 4)
    two_rows = jnp.concatenate([first, rows1])
    rows2 = row_swap(two_rows, 4)
    part_4 = ladder([(got_y2, 0, 2)], slabs, [], chunk=16)
    got_x = col_swap(jnp.concatenate([near, got_y1]), 2)
    four_rows = jnp.concatenate([two_rows, rows2])
    rows3 = row_swap(four_rows, 2)
    part_26 = ladder([(got_y1, 0, 4)], slabs, [])
    mine = jnp.concatenate([four_rows, rows3])
    other = col_swap(mine, 1)
    part_x = ladder([(got_x, 0, 8)], slabs, [], chunk=16)
    hole = hole_terms(wide, mine, other)

    def more(even, part, at, far, row, kind=F32, chunk=16):
        amps = [(even, at, 2), (got_x, far, 2)]
        starts = [[(part, at, 2), (part_x, far, 2)], [(hole, row, 4)]]
        return ladder(amps, others, starts, kind=kind, chunk=chunk)

    send_67 = more(got_y1, part_26, 2, 6, 12, BF, 8)
    back_23 = col_swap(send_67, 8).astype(F32)
    send_45 = more(got_y2, part_4, 0, 2, 8, BF)
    back_01 = col_swap(send_45, 8).astype(F32)
    full_23 = more(got_y1, part_26, 0, 4, 4)
    near_01 = col_swap((full_23 + back_23).astype(BF), 4).astype(F32)
    full_01 = more(first, part_0, 0, 0, 0)
    total = full_01 + back_01 + near_01
    last = col_swap(total[2:].astype(BF), 2).astype(F32)
    total = total[:2] + last
    occ_first = lax.dynamic_slice_in_dim(eps_occ, r * 2, 2, 0)
    occ_second = lax.dynamic_slice_in_dim(eps_occ, c, 1, 0)
    denom = (
        eps_vir[None, :, None]
        + eps_vir[None, None, :]
        - occ_first[:, None, None]
        - occ_second[:, None, None]
    )
    return ((drive.reshape(2, V, V).astype(F32) + total) / denom).reshape(2, 1, V, V)


def solution(mesh):
    placed = (
        P("row", "col", None, None),
        P("col", None, None),
        P("row", "col", None, None),
        P(),
        P(),
        P(),
    )

    return jax.shard_map(
        body, mesh=mesh, in_specs=placed, out_specs=P("row", "col", None, None), check_vma=False
    )
```

```python
import jax
import jax.numpy as jnp
from jax import lax
from jax.experimental import pallas as pl
from jax.experimental.pallas import tpu as pltpu
from jax.sharding import PartitionSpec as P


V = 128
BF = jnp.bfloat16
F32 = jnp.float32
VMEM = pl.BlockSpec(memory_space=pltpu.VMEM)
SMEM = pl.BlockSpec(memory_space=pltpu.SMEM)
HBM = pl.BlockSpec(memory_space=pltpu.HBM)
PARTS = 8


def col_swap(x, mask):
    return lax.ppermute(x, "col", [(c, c ^ mask) for c in range(16)])


def row_swap(x, mask):
    return lax.ppermute(x, "row", [(r, r ^ mask) for r in range(8)])


def params(mib):
    return pltpu.CompilerParams(vmem_limit_bytes=mib * 2**20)


def cost(flops, nbytes):
    return pl.CostEstimate(flops=flops, bytes_accessed=nbytes, transcendentals=0)


def ladder(amps, slabs, starts, pull=False, kind=F32, chunk=8):
    pairs = sum(n for _, _, n in amps)
    duos = pairs // 2
    nq = slabs.shape[0]
    half = chunk // 2
    steps = nq // chunk
    part = nq // PARTS
    namps = len(amps)
    nstart = sum(len(pieces) for pieces in starts)

    def kern(*refs):
        refs = list(refs)
        t_refs, src_ref = refs[:namps], refs[namps]
        s_refs, refs = refs[namps + 1 : namps + 1 + nstart], refs[namps + 1 + nstart :]
        o_ref = refs.pop(0)
        b_ref = refs.pop(0) if pull else src_ref
        xa, xb, acc_ref, home = refs[:4]
        copies = []
        if pull:
            pulled = pltpu.make_async_copy(t_refs[0], home, refs[5])
            pulled.start()
            for n in range(PARTS):
                span = pl.ds(n * part, part)
                copies.append(pltpu.make_async_copy(src_ref.at[span], b_ref.at[span], refs[4].at[n]))
                copies[-1].start()
        else:
            to = 0
            for ref, (_, at, n) in zip(t_refs, amps):
                home[to : to + n] = ref[at : at + n]
                to += n
        sums = [None] * pairs
        left = list(s_refs)
        for pieces in starts:
            to = 0
            for _, at, n in pieces:
                ref = left.pop(0)
                for p in range(n):
                    value = ref[at + p]
                    sums[to + p] = value if sums[to + p] is None else sums[to + p] + value
                to += n
        for p in range(pairs):
            value = jnp.zeros((V, V), F32) if sums[p] is None else sums[p]
            acc_ref[p // 2, :, (p % 2) * V : (p % 2 + 1) * V] = value

        def first(k, q, x_ref):
            two = b_ref[pl.ds(k * chunk + 2 * q, 2)].reshape(2 * V, V)
            x = lax.dot_general(
                home[...].reshape(pairs * V, V),
                two,
                (((1,), (1,)), ((), ())),
                preferred_element_type=F32,
            ).astype(BF)
            for p in range(pairs):
                xp = x[p * V : (p + 1) * V]
                g, h = p // 2, p % 2
                x_ref[g, 2 * q * V : (2 * q + 1) * V, h * V : (h + 1) * V] = xp[:, :V]
                x_ref[g, (2 * q + 1) * V : (2 * q + 2) * V, h * V : (h + 1) * V] = xp[:, V:]

        def second(k, g, x_ref):
            wide = jnp.concatenate([b_ref[k * chunk + q] for q in range(chunk)], axis=1)
            acc_ref[g] += jnp.dot(wide, x_ref[g], preferred_element_type=F32)

        def both(k1, x1, k2, x2):
            n = max(half, duos)
            for i in range(n):
                for q in range(i * half // n, (i + 1) * half // n):
                    first(k1, q, x1)
                for g in range(i * duos // n, (i + 1) * duos // n):
                    second(k2, g, x2)

        if pull:
            pulled.wait()
        ahead = max(1, chunk // part)
        for copy in copies[:ahead]:
            copy.wait()
        for q in range(half):
            first(0, q, xa)
        for copy in copies[ahead:]:
            copy.wait()

        def step(m, carry):
            both(2 * m + 1, xb, 2 * m, xa)
            both(2 * m + 2, xa, 2 * m + 1, xb)
            return carry

        lax.fori_loop(0, (steps - 2) // 2, step, 0)
        both(steps - 1, xb, steps - 2, xa)
        for g in range(duos):
            second(steps - 1, g, xb)
        for p in range(pairs):
            o_ref[p] = acc_ref[p // 2, :, (p % 2) * V : (p % 2 + 1) * V].astype(kind)

    shapes = [jax.ShapeDtypeStruct((pairs, V, V), kind)]
    scratch = [pltpu.VMEM((duos, chunk * V, 2 * V), BF)] * 2 + [pltpu.VMEM((duos, V, 2 * V), F32)]
    scratch.append(pltpu.VMEM((pairs, V, V), BF))
    arrays = [array for array, _, _ in amps] + [slabs]
    if pull:
        shapes.append(jax.ShapeDtypeStruct(slabs.shape, BF))
        scratch += [pltpu.SemaphoreType.DMA((PARTS,)), pltpu.SemaphoreType.DMA(())]
        arrays = [pltpu.with_memory_space_constraint(array, pltpu.HBM) for array in arrays]
    specs = [HBM if pull else VMEM] * len(arrays) + [VMEM] * nstart
    out = pl.pallas_call(
        kern,
        in_specs=specs,
        out_specs=[VMEM] * len(shapes),
        out_shape=shapes,
        scratch_shapes=scratch,
        compiler_params=params(8 + duos * chunk * 256 // 1024),
        cost_estimate=cost(4 * pairs * nq * V**3, slabs.size * 2),
    )(*arrays, *[array for pieces in starts for array, _, _ in pieces])
    return out if pull else out[0]


def spread_ints(ints, where):
    def kern(w_ref, h_ref, o_ref):
        r, c = w_ref[0], w_ref[1]
        line = lax.broadcasted_iota(jnp.int32, (256, 32), 0) >> 4
        pair = lax.broadcasted_iota(jnp.int32, (256, 32), 1)
        slot, ii = line >> 1, line & 1
        rows = jnp.where(pair == (ii << 4) + (c ^ (slot << 1)), 1.0, 0.0).astype(BF)
        picked = jnp.dot(rows, h_ref[...], preferred_element_type=F32).astype(BF)
        true = lax.broadcasted_iota(jnp.int32, (256, 512), 0)
        here = lax.broadcasted_iota(jnp.int32, (256, 512), 1)
        par, d, kk = here >> 8, (here >> 5) & 7, (here >> 4) & 1
        mask = (d & 1) | ((d & 2) << 1) | ((d & 4) >> 1)
        wanted = ((((r ^ mask) << 1) + kk) << 4) + (c ^ par)
        cols = jnp.where(true == wanted, 1.0, 0.0).astype(BF)
        wide = jnp.dot(picked, cols, preferred_element_type=F32)
        o_ref[...] = jnp.where((true & 15) == (here & 15), wide, 0.0).astype(BF)

    return pl.pallas_call(
        kern,
        in_specs=[SMEM, VMEM],
        out_specs=VMEM,
        out_shape=jax.ShapeDtypeStruct((256, 512), BF),
        compiler_params=params(8),
        cost_estimate=cost(10**8, 10**6),
        name="spread",
    )(where, ints)


def hole_terms(wide, mine, other, ahead):
    def kern(w_ref, m_ref, p_ref, a_ref, s_ref, o_ref):
        for ga in range(8):
            rows = slice(ga * 16, (ga + 1) * 16)
            stack = jnp.concatenate(
                [m_ref[q, rows, :] for q in range(16)] + [p_ref[q, rows, :] for q in range(16)],
                axis=0,
            )
            terms = jnp.dot(w_ref[...], stack, preferred_element_type=F32)
            for n in range(12):
                o_ref[n, rows, :] = terms[n * 16 : (n + 1) * 16]
            for n in range(4):
                value = terms[(12 + n) * 16 : (13 + n) * 16]
                s_ref[n, rows, :] = (a_ref[n, rows, :] + value).astype(BF)

    return pl.pallas_call(
        kern,
        in_specs=[VMEM] * 4,
        out_specs=[VMEM] * 2,
        out_shape=[
            jax.ShapeDtypeStruct((4, V, V), BF),
            jax.ShapeDtypeStruct((12, V, V), F32),
        ],
        compiler_params=params(8),
        cost_estimate=cost(10**9, 10**6),
        name="hole",
    )(wide, mine, other, ahead)


def body(t_amps, df_slabs, drive, hole_ints, eps_occ, eps_vir):
    r = lax.axis_index("row")
    c = lax.axis_index("col")
    where = jnp.stack([r, c]).astype(jnp.int32)
    own = t_amps.reshape(2, V, V)
    others = col_swap(df_slabs, 1)
    got_y2 = col_swap(own, 8)
    rows1 = row_swap(own, 1)
    ints = lax.dynamic_slice_in_dim(hole_ints, r * 2, 2, 0).reshape(32, 256)
    first, where, ints = lax.optimization_barrier((own, where, ints))
    wide = spread_ints(ints, where)
    part_0, slabs = ladder([(first, 0, 2)], df_slabs, [], pull=True, chunk=16)
    near = jnp.concatenate([own, got_y2])
    got_y1 = col_swap(near, 4)
    two_rows = jnp.concatenate([first, rows1])
    rows2 = row_swap(two_rows, 4)
    part_4 = ladder([(got_y2, 0, 2)], slabs, [], chunk=16)
    got_x = col_swap(jnp.concatenate([near, got_y1]), 2)
    four_rows = jnp.concatenate([two_rows, rows2])
    rows3 = row_swap(four_rows, 2)
    part_26 = ladder([(got_y1, 0, 4)], slabs, [], chunk=16)
    mine = jnp.concatenate([four_rows, rows3])
    other = col_swap(mine, 1)
    part_x = ladder([(got_x, 0, 8)], slabs, [], chunk=16)

    def more(even, part, at, far, extra=(), kind=F32):
        amps = [(even, at, 2), (got_x, far, 2)]
        starts = [[(part, at, 2), (part_x, far, 2)]] + [[piece] for piece in extra]
        return ladder(amps, others, starts, kind=kind, chunk=16)

    full_67 = more(got_y1, part_26, 2, 6)
    send_67, hole = hole_terms(wide, mine, other, full_67)
    back_23 = col_swap(send_67, 8).astype(F32)
    send_45 = more(got_y2, part_4, 0, 2, [(hole, 8, 4)], BF)
    back_01 = col_swap(send_45, 8).astype(F32)
    full_23 = more(got_y1, part_26, 0, 4, [(hole, 4, 4)])
    near_01 = col_swap((full_23 + back_23).astype(BF), 4).astype(F32)
    full_01 = more(first, part_0, 0, 0, [(hole, 0, 4)])
    total = full_01 + back_01 + near_01
    last = col_swap(total[2:].astype(BF), 2).astype(F32)
    total = total[:2] + last
    occ_first = lax.dynamic_slice_in_dim(eps_occ, r * 2, 2, 0)
    occ_second = lax.dynamic_slice_in_dim(eps_occ, c, 1, 0)
    denom = (
        eps_vir[None, :, None]
        + eps_vir[None, None, :]
        - occ_first[:, None, None]
        - occ_second[:, None, None]
    )
    return ((drive.reshape(2, V, V).astype(F32) + total) / denom).reshape(2, 1, V, V)


def solution(mesh):
    placed = (
        P("row", "col", None, None),
        P("col", None, None),
        P("row", "col", None, None),
        P(),
        P(),
        P(),
    )

    return jax.shard_map(
        body, mesh=mesh, in_specs=placed, out_specs=P("row", "col", None, None), check_vma=False
    )
```

```python
import jax
import jax.numpy as jnp
from jax import lax
from jax.experimental import pallas as pl
from jax.experimental.pallas import tpu as pltpu
from jax.sharding import PartitionSpec as P


V = 128
BF = jnp.bfloat16
F32 = jnp.float32
VMEM = pl.BlockSpec(memory_space=pltpu.VMEM)
SMEM = pl.BlockSpec(memory_space=pltpu.SMEM)
HBM = pl.BlockSpec(memory_space=pltpu.HBM)
PARTS = 8


def col_swap(x, mask):
    return lax.ppermute(x, "col", [(c, c ^ mask) for c in range(16)])


def row_swap(x, mask):
    return lax.ppermute(x, "row", [(r, r ^ mask) for r in range(8)])


def params(mib):
    return pltpu.CompilerParams(vmem_limit_bytes=mib * 2**20)


def cost(flops, nbytes):
    return pl.CostEstimate(flops=flops, bytes_accessed=nbytes, transcendentals=0)


def ladder(amps, slabs, starts, pull=False, kind=F32, chunk=8):
    pairs = sum(n for _, _, n in amps)
    duos = pairs // 2
    nq = slabs.shape[0]
    half = chunk // 2
    steps = nq // chunk
    part = nq // PARTS
    namps = len(amps)
    nstart = sum(len(pieces) for pieces in starts)

    def kern(*refs):
        refs = list(refs)
        t_refs, src_ref = refs[:namps], refs[namps]
        s_refs, refs = refs[namps + 1 : namps + 1 + nstart], refs[namps + 1 + nstart :]
        o_ref = refs.pop(0)
        b_ref = refs.pop(0) if pull else src_ref
        xa, xb, acc_ref, home = refs[:4]
        copies = []
        if pull:
            pulled = pltpu.make_async_copy(t_refs[0], home, refs[5])
            pulled.start()
            for n in range(PARTS):
                span = pl.ds(n * part, part)
                copies.append(pltpu.make_async_copy(src_ref.at[span], b_ref.at[span], refs[4].at[n]))
                copies[-1].start()
        else:
            to = 0
            for ref, (_, at, n) in zip(t_refs, amps):
                home[to : to + n] = ref[at : at + n]
                to += n
        sums = [None] * pairs
        left = list(s_refs)
        for pieces in starts:
            to = 0
            for _, at, n in pieces:
                ref = left.pop(0)
                for p in range(n):
                    value = ref[at + p]
                    sums[to + p] = value if sums[to + p] is None else sums[to + p] + value
                to += n
        for p in range(pairs):
            value = jnp.zeros((V, V), F32) if sums[p] is None else sums[p]
            acc_ref[p // 2, :, (p % 2) * V : (p % 2 + 1) * V] = value

        def first(k, q, x_ref):
            two = b_ref[pl.ds(k * chunk + 2 * q, 2)].reshape(2 * V, V)
            x = lax.dot_general(
                home[...].reshape(pairs * V, V),
                two,
                (((1,), (1,)), ((), ())),
                preferred_element_type=F32,
            ).astype(BF)
            for p in range(pairs):
                xp = x[p * V : (p + 1) * V]
                g, h = p // 2, p % 2
                x_ref[g, 2 * q * V : (2 * q + 1) * V, h * V : (h + 1) * V] = xp[:, :V]
                x_ref[g, (2 * q + 1) * V : (2 * q + 2) * V, h * V : (h + 1) * V] = xp[:, V:]

        def second(k, g, x_ref):
            wide = jnp.concatenate([b_ref[k * chunk + q] for q in range(chunk)], axis=1)
            acc_ref[g] += jnp.dot(wide, x_ref[g], preferred_element_type=F32)

        def both(k1, x1, k2, x2):
            n = max(half, duos)
            for i in range(n):
                for q in range(i * half // n, (i + 1) * half // n):
                    first(k1, q, x1)
                for g in range(i * duos // n, (i + 1) * duos // n):
                    second(k2, g, x2)

        if pull:
            pulled.wait()
        ahead = max(1, chunk // part)
        for copy in copies[:ahead]:
            copy.wait()
        for q in range(half):
            first(0, q, xa)
        for copy in copies[ahead:]:
            copy.wait()

        def step(m, carry):
            both(2 * m + 1, xb, 2 * m, xa)
            both(2 * m + 2, xa, 2 * m + 1, xb)
            return carry

        lax.fori_loop(0, (steps - 2) // 2, step, 0)
        both(steps - 1, xb, steps - 2, xa)
        for g in range(duos):
            second(steps - 1, g, xb)
        for p in range(pairs):
            o_ref[p] = acc_ref[p // 2, :, (p % 2) * V : (p % 2 + 1) * V].astype(kind)

    shapes = [jax.ShapeDtypeStruct((pairs, V, V), kind)]
    scratch = [pltpu.VMEM((duos, chunk * V, 2 * V), BF)] * 2 + [pltpu.VMEM((duos, V, 2 * V), F32)]
    scratch.append(pltpu.VMEM((pairs, V, V), BF))
    arrays = [array for array, _, _ in amps] + [slabs]
    if pull:
        shapes.append(jax.ShapeDtypeStruct(slabs.shape, BF))
        scratch += [pltpu.SemaphoreType.DMA((PARTS,)), pltpu.SemaphoreType.DMA(())]
        arrays = [pltpu.with_memory_space_constraint(array, pltpu.HBM) for array in arrays]
    specs = [HBM if pull else VMEM] * len(arrays) + [VMEM] * nstart
    out = pl.pallas_call(
        kern,
        in_specs=specs,
        out_specs=[VMEM] * len(shapes),
        out_shape=shapes,
        scratch_shapes=scratch,
        compiler_params=params(8 + duos * chunk * 256 // 1024),
        cost_estimate=cost(4 * pairs * nq * V**3, slabs.size * 2),
    )(*arrays, *[array for pieces in starts for array, _, _ in pieces])
    return out if pull else out[0]


def spread_ints(ints, where):
    def kern(w_ref, h_ref, o_ref):
        r, c = w_ref[0], w_ref[1]
        line = lax.broadcasted_iota(jnp.int32, (256, 32), 0) >> 4
        pair = lax.broadcasted_iota(jnp.int32, (256, 32), 1)
        slot, ii = line >> 1, line & 1
        rows = jnp.where(pair == (ii << 4) + (c ^ (slot << 1) ^ (slot & 4)), 1.0, 0.0).astype(BF)
        picked = jnp.dot(rows, h_ref[...], preferred_element_type=F32).astype(BF)
        true = lax.broadcasted_iota(jnp.int32, (256, 512), 0)
        here = lax.broadcasted_iota(jnp.int32, (256, 512), 1)
        par, d, kk = here >> 8, (here >> 5) & 7, (here >> 4) & 1
        mask = (d & 1) ^ (d & 2) ^ ((d & 2) << 1) ^ ((d & 4) >> 1)
        wanted = ((((r ^ mask) << 1) + kk) << 4) + (c ^ par)
        cols = jnp.where(true == wanted, 1.0, 0.0).astype(BF)
        wide = jnp.dot(picked, cols, preferred_element_type=F32)
        o_ref[...] = jnp.where((true & 15) == (here & 15), wide, 0.0).astype(BF)

    return pl.pallas_call(
        kern,
        in_specs=[SMEM, VMEM],
        out_specs=VMEM,
        out_shape=jax.ShapeDtypeStruct((256, 512), BF),
        compiler_params=params(8),
        cost_estimate=cost(10**9, 10**6),
        name="spread",
    )(where, ints)


def hole_terms(wide, mine, other, ahead):
    def kern(w_ref, m_ref, p_ref, a_ref, s_ref, o_ref):
        for ga in range(8):
            rows = slice(ga * 16, (ga + 1) * 16)
            stack = jnp.concatenate(
                [m_ref[q, rows, :] for q in range(16)] + [p_ref[q, rows, :] for q in range(16)],
                axis=0,
            )
            terms = jnp.dot(w_ref[...], stack, preferred_element_type=F32)
            for n in range(12):
                o_ref[n, rows, :] = terms[n * 16 : (n + 1) * 16]
            for n in range(4):
                value = terms[(12 + n) * 16 : (13 + n) * 16]
                s_ref[n, rows, :] = (a_ref[n, rows, :] + value).astype(BF)

    return pl.pallas_call(
        kern,
        in_specs=[VMEM] * 4,
        out_specs=[VMEM] * 2,
        out_shape=[
            jax.ShapeDtypeStruct((4, V, V), BF),
            jax.ShapeDtypeStruct((12, V, V), F32),
        ],
        compiler_params=params(8),
        cost_estimate=cost(10**9, 10**6),
        name="hole",
    )(wide, mine, other, ahead)


def body(t_amps, df_slabs, drive, hole_ints, eps_occ, eps_vir):
    r = lax.axis_index("row")
    c = lax.axis_index("col")
    where = jnp.stack([r, c]).astype(jnp.int32)
    own = t_amps.reshape(2, V, V)
    others = col_swap(df_slabs, 1)
    got_y2 = col_swap(own, 12)
    rows1 = row_swap(own, 1)
    ints = lax.dynamic_slice_in_dim(hole_ints, r * 2, 2, 0).reshape(32, 256)
    where, ints = lax.optimization_barrier((where, ints))
    wide = spread_ints(ints, where)
    first, wide = lax.optimization_barrier((own, wide))
    slabs = df_slabs
    part_0 = ladder([(first, 0, 2)], slabs, [], chunk=16)
    near = jnp.concatenate([own, got_y2])
    got_y1 = col_swap(near, 4)
    two_rows = jnp.concatenate([first, rows1])
    rows2 = row_swap(two_rows, 6)
    part_4 = ladder([(got_y2, 0, 2)], slabs, [], chunk=16)
    got_x = col_swap(jnp.concatenate([near, got_y1]), 2)
    four_rows = jnp.concatenate([two_rows, rows2])
    rows3 = row_swap(four_rows, 2)
    part_26 = ladder([(got_y1, 0, 4)], slabs, [], chunk=16)
    mine = jnp.concatenate([four_rows, rows3])
    other = col_swap(mine, 1)
    part_x = ladder([(got_x, 0, 8)], slabs, [], chunk=16)

    def more(even, part, at, far, extra=(), kind=F32):
        amps = [(even, at, 2), (got_x, far, 2)]
        starts = [[(part, at, 2), (part_x, far, 2)]] + [[piece] for piece in extra]
        return ladder(amps, others, starts, kind=kind, chunk=16)

    full_67 = more(got_y1, part_26, 2, 6)
    send_67, hole = hole_terms(wide, mine, other, full_67)
    back_23 = col_swap(send_67, 12).astype(F32)
    send_45 = more(got_y2, part_4, 0, 2, [(hole, 8, 4)], BF)
    back_01 = col_swap(send_45, 12).astype(F32)
    full_23 = more(got_y1, part_26, 0, 4, [(hole, 4, 4)])
    near_01 = col_swap((full_23 + back_23).astype(BF), 4).astype(F32)
    full_01 = more(first, part_0, 0, 0, [(hole, 0, 4)])
    total = full_01 + back_01 + near_01
    last = col_swap(total[2:].astype(BF), 2).astype(F32)
    total = total[:2] + last
    occ_first = lax.dynamic_slice_in_dim(eps_occ, r * 2, 2, 0)
    occ_second = lax.dynamic_slice_in_dim(eps_occ, c, 1, 0)
    denom = (
        eps_vir[None, :, None]
        + eps_vir[None, None, :]
        - occ_first[:, None, None]
        - occ_second[:, None, None]
    )
    return ((drive.reshape(2, V, V).astype(F32) + total) / denom).reshape(2, 1, V, V)


def solution(mesh):
    placed = (
        P("row", "col", None, None),
        P("col", None, None),
        P("row", "col", None, None),
        P(),
        P(),
        P(),
    )

    return jax.shard_map(
        body, mesh=mesh, in_specs=placed, out_specs=P("row", "col", None, None), check_vma=False
    )
```
